32 devices in a mesh: dp: 16 (over z, y, x), layer: 2 (over core).
Axes of the slice: x: 2, y: 2, z: 4, core: 2. Of those that a mesh axis runs over, the one named last changes fastest.
Arguments:
- layer_inputs: bfloat16 [2, 16384, 4096], P('layer', 'dp'), may hold values from -6 to 6
- output_grads: bfloat16 [2, 16384, 512], P('layer', 'dp'), may hold values from -6 to 6
- input_factors: bfloat16 [128, 2, 4, 4096], P('dp', 'layer'), may hold values from -0.09375 to 0.09375
- output_factors: bfloat16 [128, 2, 4, 512], P('dp', 'layer'), may hold values from -0.25 to 0.25
Outputs:
- scores: float32 [128, 16384], P(None, 'dp')
The draws below stay inside these ranges and needn't reach their ends.
All inputs are finite; a program needn't handle non-finite values.
Results may differ from the reference program's by a relative error of at most 0.0003.
Values may be sent and summed in bfloat16 or wider, within the bound.
A program may use at most 128 MiB of HBM per device.

```python
import jax
import jax.numpy as jnp
from jax import lax

D = 4096
KV = 512
RANK = 4
LAYERS = 2
TOKENS = 16384
QUERIES = 128


def shard_levels(key, extent, shards, least, high):
    gain = 1.0
    for dim, blocks in shards:
        steps = jax.random.uniform(jax.random.fold_in(jax.random.fold_in(key, 6), dim), (blocks,), jnp.float32, least / len(shards), high / len(shards))
        gain = gain * jnp.repeat(jnp.exp(steps), extent[dim] // blocks).reshape((-1,) + (1,) * (len(extent) - 1 - dim))
    return gain


def gaussian(rng, dims, deviation, most, shards=(), held_as=jnp.bfloat16):
    entries = jax.random.normal(rng, dims, jnp.float32) * deviation
    if len(shards) > 0:
        entries = shard_levels(rng, dims, shards, -0.22, 0.18) * entries
    return jnp.clip(entries, min=-most, max=most).astype(held_as)


def setup_inputs(seed: int = 0) -> dict:
    key_of = jax.random.split(jax.random.key(seed), 5)
    return {
        "layer_inputs": gaussian(key_of[0], (LAYERS, TOKENS, D), 1.0, 6.0, ((0, 2), (1, 16))),
        "output_grads": gaussian(key_of[1], (LAYERS, TOKENS, KV), 1.0, 6.0, ((0, 2), (1, 16))),
        "input_factors": gaussian(key_of[2], (QUERIES, LAYERS, RANK, D), D ** -0.5, 0.09375, ((0, 16), (1, 2))),
        "output_factors": gaussian(key_of[3], (QUERIES, LAYERS, RANK, KV), KV ** -0.5, 0.25, ((0, 16), (1, 2))),
    }


def layer_term(acts, grads, in_fac, out_fac):
    count = in_fac.shape[0]
    in_flat = in_fac.reshape(count * in_fac.shape[1], in_fac.shape[2])
    out_flat = out_fac.reshape(count * out_fac.shape[1], out_fac.shape[2])
    proj_in = lax.dot_general(acts, in_flat, (((1,), (1,)), ((), ())), preferred_element_type=jnp.float32)
    proj_out = lax.dot_general(grads, out_flat, (((1,), (1,)), ((), ())), preferred_element_type=jnp.float32)
    joined = (proj_in * proj_out).reshape(acts.shape[0], count, in_fac.shape[1])
    return jnp.sum(joined, axis=2).T


def reference(layer_inputs, output_grads, input_factors, output_factors):
    in_layers = jnp.moveaxis(input_factors, 1, 0)
    out_layers = jnp.moveaxis(output_factors, 1, 0)

    def step(total, items):
        acts, grads, in_fac, out_fac = items
        return total + layer_term(acts, grads, in_fac, out_fac), None

    start = jnp.zeros((QUERIES, TOKENS), jnp.float32)
    total, unused = lax.scan(step, start, (layer_inputs, output_grads, in_layers, out_layers))
    return total
```

```python
import functools

import jax
import jax.numpy as jnp
from jax import lax
from jax.experimental import pallas as pl
from jax.experimental.pallas import tpu as pltpu
from jax.sharding import PartitionSpec as P

MESH = pl.DeviceIdType.MESH
OWN, ACROSS_X, ACROSS_Y, DIAG = range(4)
PIECES = 2


def kernel(nz, layers, count, rank, own_ref, acts_hbm, grads_hbm, out_ref,
           slots, acts, grads, parts, load_sem, recv_sem, x_sem, y_sem, z_sem, psend_sem, precv_sem):
    me = lax.axis_index("dp")
    layer = lax.axis_index("layer")
    x, y, z = me % 2, (me // 2) % 2, me // 4
    rows, width = own_ref.shape
    half = rows // PIECES
    d_in = acts.shape[1]
    tokens = acts.shape[0]
    to_x = {"dp": me + 1 - 2 * x}
    to_y = {"dp": me + 2 - 4 * y}
    to_up = {"dp": (me + 4) % (4 * nz)}
    to_down = {"dp": (me + 4 * nz - 4) % (4 * nz)}
    has_up, has_down = z < nz - 1, z > 0

    load_acts = pltpu.make_async_copy(acts_hbm, acts, load_sem.at[0])
    load_grads = pltpu.make_async_copy(grads_hbm, grads, load_sem.at[1])
    load_acts.start()
    load_grads.start()

    barrier = pltpu.get_barrier_semaphore()
    pl.semaphore_signal(barrier, inc=1, device_id=to_x, device_id_type=MESH)
    pl.semaphore_signal(barrier, inc=1, device_id=to_y, device_id_type=MESH)
    for k in range(1, layers):
        pl.semaphore_signal(barrier, inc=1, device_id={"layer": (layer + k) % layers}, device_id_type=MESH)

    @pl.when(has_up)
    def _():
        pl.semaphore_signal(barrier, inc=1, device_id=to_up, device_id_type=MESH)

    @pl.when(has_down)
    def _():
        pl.semaphore_signal(barrier, inc=1, device_id=to_down, device_id_type=MESH)

    line_ends = (z + nz - 2) // (nz - 1) + (2 * nz - 3 - z) // (nz - 1)
    pl.semaphore_wait(barrier, 2 + layers - 1 + line_ends)

    def copy(src, target, level, piece, sem, device):
        at = target * nz + level
        return pltpu.make_async_remote_copy(
            src_ref=src,
            dst_ref=slots.at[at, pl.ds(piece * half, half), :],
            send_sem=sem,
            recv_sem=recv_sem.at[at, piece],
            device_id=device,
            device_id_type=MESH,
        )

    def held(source, level, piece):
        return slots.at[source * nz + level, pl.ds(piece * half, half), :]

    def arrived(target, level, piece):
        copy(held(target, level, piece), target, level, piece, x_sem.at[0, 0, 0], to_x).wait_recv()

    def mine(level, piece, first):
        return own_ref.at[pl.ds(piece * half, half), :] if first else held(OWN, level, piece)

    def up(level, piece, first):
        return copy(mine(level, piece, first), OWN, level, piece, z_sem.at[0, level, piece], to_up)

    def down(level, piece, first):
        return copy(mine(level, piece, first), OWN, level, piece, z_sem.at[1, level, piece], to_down)

    def side_x(level, piece, first):
        return copy(mine(level, piece, first), ACROSS_X, level, piece, x_sem.at[0, level, piece], to_x)

    def side_y(level, piece, first):
        return copy(mine(level, piece, first), ACROSS_Y, level, piece, y_sem.at[0, level, piece], to_y)

    def turn_x(level):
        return copy(held(ACROSS_Y, level, 0), DIAG, level, 0, x_sem.at[1, level, 0], to_x)

    def turn_y(level):
        return copy(held(ACROSS_X, level, 1), DIAG, level, 1, y_sem.at[1, level, 1], to_y)

    def at_distance(step, act):
        if step == 0:
            act(z, None)
            return

        @pl.when(z >= step)
        def _():
            act(z - step, True)

        @pl.when(z + step < nz)
        def _():
            act(z + step, False)

    def turn(level, unused):
        arrived(ACROSS_Y, level, 0)
        turn_x(level).start()
        arrived(ACROSS_X, level, 1)
        turn_y(level).start()

    for piece in range(PIECES):
        @pl.when(has_up)
        def _():
            up(z, piece, True).start()

        @pl.when(has_down)
        def _():
            down(z, piece, True).start()

        side_x(z, piece, True).start()
        side_y(z, piece, True).start()
    slots[OWN * nz + z] = own_ref[...]

    for step in range(1, nz):
        for piece in range(PIECES):
            def relay(level, from_below):
                arrived(OWN, level, piece)
                if from_below:
                    @pl.when(has_up)
                    def _():
                        up(level, piece, False).start()
                else:
                    @pl.when(has_down)
                    def _():
                        down(level, piece, False).start()
                side_x(level, piece, False).start()
                side_y(level, piece, False).start()

            at_distance(step, relay)
        at_distance(step - 1, turn)
    at_distance(nz - 1, turn)

    chunk = min(256, tokens)

    def scores_of(first, classes):
        blocks = classes * nz

        def body(i, carry):
            cols = pl.ds(pl.multiple_of(i * chunk, chunk), chunk)
            left = slots[first * nz:first * nz + blocks]
            left = left.reshape(blocks * rows, width)
            dims = (((1,), (1,)), ((), ()))
            proj_in = lax.dot_general(left[:, :d_in], acts[cols, :], dims, preferred_element_type=jnp.float32)
            proj_out = lax.dot_general(left[:, d_in:], grads[cols, :], dims, preferred_element_type=jnp.float32)
            joined = (proj_in * proj_out).reshape(blocks, rank, count, chunk)
            term = jnp.sum(joined, axis=1).reshape(blocks * count, chunk)
            parts[layer, first * nz * count:(first * nz + blocks) * count, cols] = term
            return carry

        lax.fori_loop(0, tokens // chunk, body, 0)

    def share(stage, first, classes, k):
        span = pl.ds(first * nz * count, classes * nz * count)
        return pltpu.make_async_remote_copy(
            src_ref=parts.at[layer, span, :],
            dst_ref=parts.at[layer, span, :],
            send_sem=psend_sem.at[stage, k],
            recv_sem=precv_sem.at[stage, layer],
            device_id={"layer": (layer + k) % layers},
            device_id_type=MESH,
        )

    def shared(stage, first, classes, k):
        source = (layer + k) % layers
        span = pl.ds(first * nz * count, classes * nz * count)
        pltpu.make_async_remote_copy(
            src_ref=parts.at[source, span, :],
            dst_ref=parts.at[source, span, :],
            send_sem=psend_sem.at[stage, k],
            recv_sem=precv_sem.at[stage, source],
            device_id={"layer": source},
            device_id_type=MESH,
        ).wait_recv()

    def finish(first, classes):
        for kind in range(first, first + classes):
            col = ((1 - y) if kind in (ACROSS_Y, DIAG) else y) * 2
            col = col + ((1 - x) if kind in (ACROSS_X, DIAG) else x)
            for level in range(nz):
                at = (kind * nz + level) * count
                total = parts[0, at:at + count, :]
                for other in range(1, layers):
                    total = total + parts[other, at:at + count, :]
                out_ref[pl.ds(pl.multiple_of((level * 4 + col) * count, count), count), :] = total

    for step in range(nz):
        def rest(level, unused):
            arrived(ACROSS_X, level, 0)
            arrived(ACROSS_Y, level, 1)

        at_distance(step, rest)
    load_acts.wait()
    load_grads.wait()
    scores_of(OWN, 3)
    for k in range(1, layers):
        share(0, OWN, 3, k).start()

    for step in range(nz):
        def last(level, unused):
            arrived(DIAG, level, 0)
            arrived(DIAG, level, 1)

        at_distance(step, last)
    scores_of(DIAG, 1)
    for k in range(1, layers):
        shared(0, OWN, 3, k)
    finish(OWN, 3)
    for k in range(1, layers):
        share(1, DIAG, 1, k).start()
    for k in range(1, layers):
        shared(1, DIAG, 1, k)
    finish(DIAG, 1)

    for step in range(nz):
        def sent(level, from_below):
            for piece in range(PIECES):
                if from_below is not False:
                    @pl.when(has_up)
                    def _():
                        up(level, piece, step == 0).wait_send()
                if from_below is not True:
                    @pl.when(has_down)
                    def _():
                        down(level, piece, step == 0).wait_send()
                side_x(level, piece, step == 0).wait_send()
                side_y(level, piece, step == 0).wait_send()
            turn_x(level).wait_send()
            turn_y(level).wait_send()

        at_distance(step, sent)
    for k in range(1, layers):
        share(0, OWN, 3, k).wait_send()
        share(1, DIAG, 1, k).wait_send()


def shards(nz, layers, layer_inputs, output_grads, input_factors, output_factors):
    count, _, rank, d_in = input_factors.shape
    d_out = output_factors.shape[3]
    tokens = layer_inputs.shape[1]
    rows, width = count * rank, d_in + d_out
    own = jnp.concatenate([input_factors[:, 0], output_factors[:, 0]], axis=2)
    own = jnp.swapaxes(own, 0, 1).reshape(rows, width)
    queries = 4 * nz * count
    dma = pltpu.SemaphoreType.DMA
    return pl.pallas_call(
        functools.partial(kernel, nz, layers, count, rank),
        out_shape=jax.ShapeDtypeStruct((queries, tokens), jnp.float32),
        in_specs=[
            pl.BlockSpec(memory_space=pltpu.VMEM),
            pl.BlockSpec(memory_space=pl.ANY),
            pl.BlockSpec(memory_space=pl.ANY),
        ],
        out_specs=pl.BlockSpec(memory_space=pltpu.VMEM),
        scratch_shapes=[
            pltpu.VMEM((4 * nz, rows, width), jnp.bfloat16),
            pltpu.VMEM((tokens, d_in), jnp.bfloat16),
            pltpu.VMEM((tokens, d_out), jnp.bfloat16),
            pltpu.VMEM((layers, queries, tokens), jnp.float32),
            dma((2,)),
            dma((4 * nz, PIECES)),
            dma((2, nz, PIECES)),
            dma((2, nz, PIECES)),
            dma((2, nz, PIECES)),
            dma((2, layers)),
            dma((2, layers)),
        ],
        compiler_params=pltpu.CompilerParams(
            collective_id=0, has_side_effects=True, vmem_limit_bytes=60 * 1024 * 1024
        ),
    )(own, layer_inputs[0], output_grads[0])


def solution(mesh):
    in_specs = (
        P("layer", "dp", None),
        P("layer", "dp", None),
        P("dp", "layer", None, None),
        P("dp", "layer", None, None),
    )
    body = functools.partial(shards, mesh.shape["dp"] // 4, mesh.shape["layer"])
    return jax.shard_map(body, mesh=mesh, in_specs=in_specs, out_specs=P(None, "dp"), check_vma=False)
```

```python
import functools

import jax
import jax.numpy as jnp
from jax import lax
from jax.experimental import pallas as pl
from jax.experimental.pallas import tpu as pltpu
from jax.sharding import PartitionSpec as P

MESH = pl.DeviceIdType.MESH
OWN, ACROSS_X, ACROSS_Y, DIAG = range(4)
PIECES = 4


def kernel(nz, layers, count, rank, own_ref, acts_hbm, grads_hbm, out_ref,
           slots, acts, grads, parts, load_sem, recv_sem, x_sem, y_sem, z_sem, psend_sem, precv_sem):
    me = lax.axis_index("dp")
    layer = lax.axis_index("layer")
    x, y, z = me % 2, (me // 2) % 2, me // 4
    rows, width = own_ref.shape
    half = rows // PIECES
    d_in = acts.shape[1]
    tokens = acts.shape[0]
    to_x = {"dp": me + 1 - 2 * x}
    to_y = {"dp": me + 2 - 4 * y}
    to_up = {"dp": (me + 4) % (4 * nz)}
    to_down = {"dp": (me + 4 * nz - 4) % (4 * nz)}
    has_up, has_down = z < nz - 1, z > 0

    load_acts = pltpu.make_async_copy(acts_hbm, acts, load_sem.at[0])
    load_grads = pltpu.make_async_copy(grads_hbm, grads, load_sem.at[1])
    load_acts.start()
    load_grads.start()

    barrier = pltpu.get_barrier_semaphore()
    pl.semaphore_signal(barrier, inc=1, device_id=to_x, device_id_type=MESH)
    pl.semaphore_signal(barrier, inc=1, device_id=to_y, device_id_type=MESH)
    for k in range(1, layers):
        pl.semaphore_signal(barrier, inc=1, device_id={"layer": (layer + k) % layers}, device_id_type=MESH)

    @pl.when(has_up)
    def _():
        pl.semaphore_signal(barrier, inc=1, device_id=to_up, device_id_type=MESH)

    @pl.when(has_down)
    def _():
        pl.semaphore_signal(barrier, inc=1, device_id=to_down, device_id_type=MESH)

    line_ends = (z + nz - 2) // (nz - 1) + (2 * nz - 3 - z) // (nz - 1)
    pl.semaphore_wait(barrier, 2 + layers - 1 + line_ends)

    def copy(src, target, level, piece, sem, device):
        at = target * nz + level
        return pltpu.make_async_remote_copy(
            src_ref=src,
            dst_ref=slots.at[at, pl.ds(piece * half, half), :],
            send_sem=sem,
            recv_sem=recv_sem.at[at, piece],
            device_id=device,
            device_id_type=MESH,
        )

    def held(source, level, piece):
        return slots.at[source * nz + level, pl.ds(piece * half, half), :]

    def arrived(target, level, piece):
        copy(held(target, level, piece), target, level, piece, x_sem.at[0, 0, 0], to_x).wait_recv()

    def mine(level, piece, first):
        return own_ref.at[pl.ds(piece * half, half), :] if first else held(OWN, level, piece)

    def up(level, piece, first):
        return copy(mine(level, piece, first), OWN, level, piece, z_sem.at[0, level, piece], to_up)

    def down(level, piece, first):
        return copy(mine(level, piece, first), OWN, level, piece, z_sem.at[1, level, piece], to_down)

    def side_x(level, piece, first):
        return copy(mine(level, piece, first), ACROSS_X, level, piece, x_sem.at[0, level, piece], to_x)

    def side_y(level, piece, first):
        return copy(mine(level, piece, first), ACROSS_Y, level, piece, y_sem.at[0, level, piece], to_y)

    def side_turn(level, piece):
        if piece < PIECES // 2:
            return copy(held(ACROSS_Y, level, piece), DIAG, level, piece, x_sem.at[1, level, piece], to_x)
        return copy(held(ACROSS_X, level, piece), DIAG, level, piece, y_sem.at[1, level, piece], to_y)

    def at_distance(step, act):
        if step == 0:
            act(z, None)
            return

        @pl.when(z >= step)
        def _():
            act(z - step, True)

        @pl.when(z + step < nz)
        def _():
            act(z + step, False)

    def turn(step, piece):
        def act(level, unused):
            arrived(ACROSS_Y if piece < PIECES // 2 else ACROSS_X, level, piece)
            side_turn(level, piece).start()

        at_distance(step, act)

    order = [p for two in zip(range(PIECES // 2), range(PIECES // 2, PIECES)) for p in two]

    for piece in range(PIECES):
        @pl.when(has_up)
        def _():
            up(z, piece, True).start()

        @pl.when(has_down)
        def _():
            down(z, piece, True).start()

        side_x(z, piece, True).start()
        side_y(z, piece, True).start()
    slots[OWN * nz + z] = own_ref[...]

    for step in range(1, nz):
        for piece in range(PIECES):
            def relay(level, from_below):
                arrived(OWN, level, piece)
                if from_below:
                    @pl.when(has_up)
                    def _():
                        up(level, piece, False).start()
                else:
                    @pl.when(has_down)
                    def _():
                        down(level, piece, False).start()
                side_x(level, piece, False).start()
                side_y(level, piece, False).start()

            at_distance(step, relay)
            turn(step - 1, order[piece])
    for piece in order:
        turn(nz - 1, piece)

    chunk = min(256, tokens)

    def scores_of(first, classes):
        blocks = classes * nz

        def body(i, carry):
            cols = pl.ds(pl.multiple_of(i * chunk, chunk), chunk)
            left = slots[first * nz:first * nz + blocks]
            left = left.reshape(blocks * rows, width)
            dims = (((1,), (1,)), ((), ()))
            proj_in = lax.dot_general(left[:, :d_in], acts[cols, :], dims, preferred_element_type=jnp.float32)
            proj_out = lax.dot_general(left[:, d_in:], grads[cols, :], dims, preferred_element_type=jnp.float32)
            joined = (proj_in * proj_out).reshape(blocks, rank, count, chunk)
            term = jnp.sum(joined, axis=1).reshape(blocks * count, chunk)
            parts[layer, first * nz * count:(first * nz + blocks) * count, cols] = term
            return carry

        lax.fori_loop(0, tokens // chunk, body, 0)

    def share(stage, first, classes, k):
        span = pl.ds(first * nz * count, classes * nz * count)
        return pltpu.make_async_remote_copy(
            src_ref=parts.at[layer, span, :],
            dst_ref=parts.at[layer, span, :],
            send_sem=psend_sem.at[stage, k],
            recv_sem=precv_sem.at[stage, layer],
            device_id={"layer": (layer + k) % layers},
            device_id_type=MESH,
        )

    def shared(stage, first, classes, k):
        source = (layer + k) % layers
        span = pl.ds(first * nz * count, classes * nz * count)
        pltpu.make_async_remote_copy(
            src_ref=parts.at[source, span, :],
            dst_ref=parts.at[source, span, :],
            send_sem=psend_sem.at[stage, k],
            recv_sem=precv_sem.at[stage, source],
            device_id={"layer": source},
            device_id_type=MESH,
        ).wait_recv()

    def finish(first, classes):
        for kind in range(first, first + classes):
            col = ((1 - y) if kind in (ACROSS_Y, DIAG) else y) * 2
            col = col + ((1 - x) if kind in (ACROSS_X, DIAG) else x)
            for level in range(nz):
                at = (kind * nz + level) * count
                total = parts[0, at:at + count, :]
                for other in range(1, layers):
                    total = total + parts[other, at:at + count, :]
                out_ref[pl.ds(pl.multiple_of((level * 4 + col) * count, count), count), :] = total

    for step in range(nz):
        def rest(level, unused):
            for piece in range(PIECES):
                arrived(ACROSS_X if piece < PIECES // 2 else ACROSS_Y, level, piece)

        at_distance(step, rest)
    load_acts.wait()
    load_grads.wait()
    scores_of(OWN, 3)
    for k in range(1, layers):
        share(0, OWN, 3, k).start()

    for step in range(nz):
        def last(level, unused):
            for piece in range(PIECES):
                arrived(DIAG, level, piece)

        at_distance(step, last)
    scores_of(DIAG, 1)
    for k in range(1, layers):
        shared(0, OWN, 3, k)
    finish(OWN, 3)
    for k in range(1, layers):
        share(1, DIAG, 1, k).start()
    for k in range(1, layers):
        shared(1, DIAG, 1, k)
    finish(DIAG, 1)

    for step in range(nz):
        def sent(level, from_below):
            for piece in range(PIECES):
                if from_below is not False:
                    @pl.when(has_up)
                    def _():
                        up(level, piece, step == 0).wait_send()
                if from_below is not True:
                    @pl.when(has_down)
                    def _():
                        down(level, piece, step == 0).wait_send()
                side_x(level, piece, step == 0).wait_send()
                side_y(level, piece, step == 0).wait_send()
                side_turn(level, piece).wait_send()

        at_distance(step, sent)
    for k in range(1, layers):
        share(0, OWN, 3, k).wait_send()
        share(1, DIAG, 1, k).wait_send()


def shards(nz, layers, layer_inputs, output_grads, input_factors, output_factors):
    count, _, rank, d_in = input_factors.shape
    d_out = output_factors.shape[3]
    tokens = layer_inputs.shape[1]
    rows, width = count * rank, d_in + d_out
    own = jnp.concatenate([input_factors[:, 0], output_factors[:, 0]], axis=2)
    own = jnp.swapaxes(own, 0, 1).reshape(rows, width)
    queries = 4 * nz * count
    dma = pltpu.SemaphoreType.DMA
    return pl.pallas_call(
        functools.partial(kernel, nz, layers, count, rank),
        out_shape=jax.ShapeDtypeStruct((queries, tokens), jnp.float32),
        in_specs=[
            pl.BlockSpec(memory_space=pltpu.VMEM),
            pl.BlockSpec(memory_space=pl.ANY),
            pl.BlockSpec(memory_space=pl.ANY),
        ],
        out_specs=pl.BlockSpec(memory_space=pltpu.VMEM),
        scratch_shapes=[
            pltpu.VMEM((4 * nz, rows, width), jnp.bfloat16),
            pltpu.VMEM((tokens, d_in), jnp.bfloat16),
            pltpu.VMEM((tokens, d_out), jnp.bfloat16),
            pltpu.VMEM((layers, queries, tokens), jnp.float32),
            dma((2,)),
            dma((4 * nz, PIECES)),
            dma((2, nz, PIECES)),
            dma((2, nz, PIECES)),
            dma((2, nz, PIECES)),
            dma((2, layers)),
            dma((2, layers)),
        ],
        compiler_params=pltpu.CompilerParams(
            collective_id=0, has_side_effects=True, vmem_limit_bytes=60 * 1024 * 1024
        ),
    )(own, layer_inputs[0], output_grads[0])


def solution(mesh):
    in_specs = (
        P("layer", "dp", None),
        P("layer", "dp", None),
        P("dp", "layer", None, None),
        P("dp", "layer", None, None),
    )
    body = functools.partial(shards, mesh.shape["dp"] // 4, mesh.shape["layer"])
    return jax.shard_map(body, mesh=mesh, in_specs=in_specs, out_specs=P(None, "dp"), check_vma=False)
```
